32 devices in a mesh: grp: 4 (over y, x), blk: 8 (over z, core).
Axes of the slice: x: 2, y: 2, z: 4, core: 2. Of those that a mesh axis runs over, the one named last changes fastest.
Arguments:
- data: bfloat16 [256, 65536], P('blk'), may hold values from -8 to 8
- labels: int32 [256], P('blk'), may hold values from -1 to 1, as said below
- order: int32 [8, 4], P('blk'), may hold values from 0 to 3, each once within a row
- reg_index: int32 [4], P('grp'), parts along dimension 0, may hold values from 0 to 5
Outputs:
- dual: float32 [1024], P(('grp', 'blk')), parts along dimension 0
- margins: float32 [1024], P(('grp', 'blk')), parts along dimension 0
- gap: float32 [4], P('grp'), parts along dimension 0
The draws below stay inside these ranges and needn't reach their ends.
There are 4 independent parts, one for each index of `grp`. The reference program is written for one: setup_inputs(seed, part) draws one part's arguments, and reference() takes and returns one part's arrays. A program takes and returns all parts, laid end to end along the dimension named above; an argument that names none is the same for every part. Nothing has to cross between parts.
Inputs may be any that keep to these rules, and one draw needn't show every extreme that they name: `labels`: each entry is -1 or 1.
All inputs are finite; a program needn't handle non-finite values.
Results may differ from the reference program's by a relative error of at most 0.00055.
Values sent between devices are 32-bit elements; how exact they have to be, the bound alone decides.
No kernel may reach another device: no remote copies, remote signals or barrier semaphores. Data moves between devices by JAX's collectives and lax.ppermute only.
A program may use at most 64 MiB of HBM per device.

```python
import math
import jax
import jax.numpy as jnp
from jax import lax

F = 65536
ROWS_DEV = 32
NBLOCKS = 4
ROUNDS = 2
SAMPLES = 256
N_BLK = 8


def common_labels(key):
    return 2 * jax.random.randint(jax.random.fold_in(key, 7), (SAMPLES,), 0, 2) - 1


def draw_labels(key, part):
    return common_labels(key).astype(jnp.int32)


def draw_data(key, part):
    label_signs = common_labels(key).astype(jnp.float32)
    row_index = jnp.arange(SAMPLES, dtype=jnp.int32)
    groups = row_index * 8 // SAMPLES
    one_hot = (groups[:, None] == jnp.arange(8, dtype=jnp.int32)[None, :]).astype(jnp.float32)
    shared_directions = jax.random.normal(jax.random.fold_in(key, 11), (64, F), jnp.float32)
    noise = jax.random.normal(jax.random.fold_in(key, 8), (SAMPLES, F), jnp.float32)
    directions = jax.random.normal(jax.random.fold_in(key, 9), (8, F), jnp.float32)
    loadings = jax.random.normal(jax.random.fold_in(key, 12), (SAMPLES, 64), jnp.float32)
    signal = jnp.dot(one_hot, directions, precision=lax.Precision.HIGHEST)
    shared = math.sqrt(1.5 / 64.0) * jnp.dot(loadings, shared_directions, precision=lax.Precision.HIGHEST)
    values = noise + 0.5 * label_signs[:, None] * signal + shared
    return jnp.clip(values, -8.0, 8.0).astype(jnp.bfloat16)


def setup_inputs(seed: int = 0, part: int = 0) -> dict:
    key_list = jax.random.split(jax.random.key(seed), 5)
    part_splits = jax.random.split(jax.random.fold_in(key_list[4], part), 5)
    data = draw_data(jax.random.fold_in(key_list[4], 71), part)
    labels = draw_labels(jax.random.fold_in(key_list[4], 71), part)
    order = jax.vmap(lambda own: jax.random.permutation(own, NBLOCKS))(jax.random.split(key_list[2], N_BLK)).reshape((N_BLK, NBLOCKS)).astype(jnp.int32)
    reg_index = jax.random.randint(part_splits[3], (1,), 0, 6).astype(jnp.int32)
    return dict(data=data, labels=labels, order=order, reg_index=reg_index)


def local_round(block_data_all, signs, dual, order_row, weights, reg_total, sigma_prime, squared):
    block_rows = block_data_all.shape[0] // NBLOCKS
    feature_scale = 1.0 / math.sqrt(block_data_all.shape[1])
    local_weights = weights
    dual_change = jnp.zeros_like(dual)
    for position in range(NBLOCKS):
        offset = (order_row[position] * block_rows).astype(jnp.int32)
        block_data = lax.dynamic_slice_in_dim(block_data_all, offset, block_rows, 0)
        block_signs = lax.dynamic_slice_in_dim(signs, offset, block_rows, 0)
        block_dual = lax.dynamic_slice_in_dim(dual, offset, block_rows, 0)
        block_change = lax.dynamic_slice_in_dim(dual_change, offset, block_rows, 0)
        block_norms = lax.dynamic_slice_in_dim(squared, offset, block_rows, 0)
        rounded = local_weights.astype(jnp.bfloat16)
        score = feature_scale * jnp.dot(block_data, rounded, preferred_element_type=jnp.float32)
        current = block_dual + block_change
        updated = jnp.clip(current + reg_total * (1.0 - block_signs * score) / (sigma_prime * block_norms), 0.0, 1.0)
        change = updated - current
        dual_change = lax.dynamic_update_slice_in_dim(dual_change, block_change + change, offset, 0)
        coefficient = (block_signs * change).astype(jnp.bfloat16)
        local_weights = local_weights + sigma_prime * feature_scale / reg_total * jnp.dot(coefficient, block_data, preferred_element_type=jnp.float32)
    coefficient = (signs * dual_change).astype(jnp.bfloat16)
    delta = feature_scale / reg_total * jnp.dot(coefficient, block_data_all, preferred_element_type=jnp.float32)
    return (dual_change, delta)

def reference(data, labels, order, reg_index):
    feature_count = data.shape[1]
    feature_scale = 1.0 / math.sqrt(feature_count)
    samples_all = data.shape[0]
    reg_strength = 0.04 * jnp.exp(0.5 * math.log(2.0) * reg_index[0].astype(jnp.float32))
    reg_total = reg_strength * samples_all
    sigma_prime = jnp.float32(N_BLK)
    signs = labels.astype(jnp.float32)
    wide = data.astype(jnp.float32)
    squared = lax.optimization_barrier(jnp.sum(wide * wide, axis=1)) / feature_count + 1e-06
    split_data = data.reshape(N_BLK, ROWS_DEV, feature_count)
    split_signs = signs.reshape(N_BLK, ROWS_DEV)
    split_norms = squared.reshape(N_BLK, ROWS_DEV)
    weights = jnp.zeros((feature_count,), jnp.float32)
    dual = jnp.zeros((N_BLK, ROWS_DEV), jnp.float32)
    mapped = jax.vmap(local_round, in_axes=(0, 0, 0, 0, None, None, None, 0))
    for round_index in range(ROUNDS):
        dual_change, delta = mapped(split_data, split_signs, dual, order, weights, reg_total, sigma_prime, split_norms)
        weights = weights + lax.optimization_barrier(jnp.sum(delta, axis=0))
        dual = dual + dual_change
    dual = dual.reshape(samples_all)
    margins = feature_scale * jnp.dot(data, weights.astype(jnp.bfloat16), preferred_element_type=jnp.float32)
    hinge = jnp.maximum(0.0, 1.0 - signs * margins)
    gap = reg_strength * jnp.sum(weights * weights) + (jnp.sum(hinge) - jnp.sum(dual)) / samples_all
    return (dual, margins, gap.reshape(1))
```

```python
import functools
import math

import jax
import jax.numpy as jnp
from jax import lax
from jax.experimental import pallas as pl
from jax.experimental.pallas import tpu as pltpu
from jax.sharding import PartitionSpec as P

ROUNDS = 2
HALF = 8
LOADS = 8

F32 = jnp.float32
BF16 = jnp.bfloat16
NT = (((1,), (1,)), ((), ()))
NN = (((1,), (0,)), ((), ()))


def regularization(reg_ref, samples):
    index = jnp.full((1, 1), reg_ref[0], jnp.int32).astype(F32)
    lam = 0.04 * jnp.exp(0.5 * math.log(2.0) * index)
    return lam, lam * samples


def ascend(gram, order_ref, signs, dual, score, reg_total, sigma, features):
    rows = gram.shape[0]
    blocks = order_ref.shape[1]
    eye = lax.broadcasted_iota(jnp.int32, (rows, rows), 0) == lax.broadcasted_iota(
        jnp.int32, (rows, rows), 1
    )
    block_of = lax.broadcasted_iota(jnp.int32, (1, rows), 1) // (rows // blocks)
    squared = jnp.sum(jnp.where(eye, gram, 0.0), axis=0, keepdims=True) / features + 1e-06
    rate = reg_total / (sigma * squared)
    couple = gram * (sigma / features / reg_total)
    change = jnp.zeros_like(dual)
    for position in range(blocks):
        current = dual + change
        updated = jnp.clip(current + rate * (1.0 - signs * score), 0.0, 1.0)
        step = jnp.where(block_of == order_ref[0, position], updated - current, 0.0)
        change = change + step
        if position < blocks - 1:
            coefficient = (signs * step).astype(BF16).astype(F32)
            column = jnp.sum(jnp.where(eye, coefficient, 0.0), axis=1, keepdims=True)
            score = score + jnp.sum(couple * column, axis=0, keepdims=True)
    return change


def weight_change(full, x_ref, keep_ref, send_ref, core, scale):
    rows, features = x_ref.shape
    segments = 2 * HALF
    length = features // segments
    depth = segments * rows
    spread = (
        lax.broadcasted_iota(jnp.int32, (rows, depth), 1) % rows
        == lax.broadcasted_iota(jnp.int32, (rows, depth), 0)
    )
    left = jnp.broadcast_to(full, (segments, rows)).astype(BF16)
    wide = lax.dot_general(
        left, jnp.where(spread, 1.0, 0.0).astype(BF16), NN, preferred_element_type=F32
    )
    segment_of = lax.broadcasted_iota(jnp.int32, (segments, depth), 1) // rows
    wanted = (lax.broadcasted_iota(jnp.int32, (segments, depth), 0) + core * HALF) % segments
    wide = jnp.where(segment_of == wanted, wide, 0.0).astype(BF16)
    width = min(length, 512)
    for begin in range(0, length, width):
        stacked = jnp.concatenate(
            [x_ref[:, g * length + begin : g * length + begin + width] for g in range(segments)],
            axis=0,
        )
        part = scale * lax.dot_general(wide, stacked, NN, preferred_element_type=F32)
        keep_ref[:, begin : begin + width] = part[:HALF]
        send_ref[:, begin : begin + width] = part[HALF:]


def scores(x_ref, low, high):
    rows, features = x_ref.shape
    segments = 2 * HALF
    length = features // segments
    total = jnp.zeros((HALF, rows), F32)
    row = lax.broadcasted_iota(jnp.int32, (HALF, rows), 0)
    for g in range(segments):
        half = low if g < HALF else high
        part = lax.dot_general(
            half, x_ref[:, g * length : (g + 1) * length], NT, preferred_element_type=F32
        )
        total = total + jnp.where(row == g % HALF, part, 0.0)
    return jnp.sum(total, axis=0, keepdims=True)


def first_kernel(samples, sigma, order_ref, reg_ref, core_ref, label_ref, data_ref,
                 keep_ref, send_ref, gram_ref, dual_ref, x_ref, arrived):
    rows, features = x_ref.shape
    width = features // LOADS
    copies = [
        pltpu.make_async_copy(
            data_ref.at[:, pl.ds(k * width, width)],
            x_ref.at[:, pl.ds(k * width, width)],
            arrived.at[k],
        )
        for k in range(LOADS)
    ]
    for copy in copies:
        copy.start()
    gram = jnp.zeros((rows, rows), F32)
    for k in range(LOADS):
        copies[k].wait()
        piece = x_ref[:, k * width : (k + 1) * width]
        gram = gram + lax.dot_general(piece, piece, NT, preferred_element_type=F32)
    gram_ref[...] = gram
    signs = label_ref[...].astype(F32)
    _, reg_total = regularization(reg_ref, samples)
    none = jnp.zeros((1, rows), F32)
    change = ascend(gram, order_ref, signs, none, none, reg_total, sigma, features)
    dual_ref[...] = change
    scale = 1.0 / math.sqrt(features) / reg_total
    weight_change((signs * change).astype(BF16), x_ref, keep_ref, send_ref, core_ref[0], scale)


def halves(own, other, core):
    low = jnp.where(core == 0, own, other)
    high = jnp.where(core == 0, other, own)
    return low, high


def next_kernel(samples, sigma, order_ref, reg_ref, core_ref, label_ref, own_ref, other_ref,
                gram_ref, old_dual_ref, x_ref, keep_ref, send_ref, dual_ref):
    rows, features = x_ref.shape
    signs = label_ref[...].astype(F32)
    _, reg_total = regularization(reg_ref, samples)
    low, high = halves(own_ref[...], other_ref[...], core_ref[0])
    score = 1.0 / math.sqrt(features) * scores(x_ref, low.astype(BF16), high.astype(BF16))
    dual = old_dual_ref[...]
    change = ascend(
        gram_ref[...], order_ref, signs, dual, score, reg_total, sigma, features
    )
    dual_ref[...] = dual + change
    scale = 1.0 / math.sqrt(features) / reg_total
    weight_change((signs * change).astype(BF16), x_ref, keep_ref, send_ref, core_ref[0], scale)


def last_kernel(samples, reg_ref, core_ref, label_ref, own_ref, other_ref, dual_ref, x_ref,
                margin_ref, share_ref, norm_ref):
    rows, features = x_ref.shape
    signs = label_ref[...].astype(F32)
    lam, _ = regularization(reg_ref, samples)
    low, high = halves(own_ref[...], other_ref[...], core_ref[0])
    margins = 1.0 / math.sqrt(features) * scores(x_ref, low.astype(BF16), high.astype(BF16))
    margin_ref[...] = margins
    hinge = jnp.maximum(0.0, 1.0 - signs * margins)
    share = jnp.sum(hinge - dual_ref[...], axis=1, keepdims=True)
    share_ref[...] = jnp.broadcast_to(share, share_ref.shape)
    norm = jnp.sum(low * low + high * high, axis=0, keepdims=True)
    norm_ref[...] = lam * jnp.sum(norm, axis=1, keepdims=True)


def gap_kernel(samples, peers, share_ref, norm_ref, gap_ref):
    total = share_ref[0:1, 0:1]
    step = share_ref.shape[0] // peers
    for k in range(1, peers):
        total = total + share_ref[k * step : k * step + 1, 0:1]
    gap_ref[...] = norm_ref[...] + total / samples


def swap(value, peers, partner):
    return lax.ppermute(value, "blk", [(i, partner(i)) for i in range(peers)])


def all_reduce(keep, send, peers):
    chips = peers // 2
    own = keep + swap(send, peers, lambda i: i ^ 1)
    mask = 1
    while mask < chips:
        own = own + swap(own, peers, lambda i: i ^ (2 * mask))
        mask = 2 * mask + 1
    return own, swap(own, peers, lambda i: i ^ 1)


def call(body, outs, spaces, scratch=()):
    return pl.pallas_call(
        body,
        out_shape=[jax.ShapeDtypeStruct(shape, F32) for shape in outs],
        in_specs=[pl.BlockSpec(memory_space=space) for space in spaces],
        out_specs=[pl.BlockSpec(memory_space=pltpu.VMEM) for _ in outs],
        scratch_shapes=list(scratch),
    )


def shards(data, labels, order, reg_index):
    peers = lax.axis_size("blk")
    rows, features = data.shape
    samples = rows * peers
    sigma = float(peers)
    half = (HALF, features // 2 // HALF)
    core = (lax.axis_index("blk") % 2).astype(jnp.int32).reshape(1)
    label_row = labels.reshape(1, rows)
    S, V, A = pltpu.SMEM, pltpu.VMEM, pl.ANY
    keep, send, gram, dual = call(
        functools.partial(first_kernel, samples, sigma),
        [half, half, (rows, rows), (1, rows)],
        [S, S, S, V, A],
        [pltpu.VMEM((rows, features), BF16), pltpu.SemaphoreType.DMA((LOADS,))],
    )(order, reg_index, core, label_row, data)
    own, other = all_reduce(keep, send, peers)
    for _ in range(ROUNDS - 1):
        keep, send, dual = call(
            functools.partial(next_kernel, samples, sigma),
            [half, half, (1, rows)],
            [S, S, S, V, V, V, V, V, V],
        )(order, reg_index, core, label_row, own, other, gram, dual, data)
        more, rest = all_reduce(keep, send, peers)
        own, other = own + more, other + rest
    margins, share, norm = call(
        functools.partial(last_kernel, samples),
        [(1, rows), (8 * peers, 128), (1, 1)],
        [S, S, V, V, V, V, V],
    )(reg_index, core, label_row, own, other, dual, data)
    share = lax.all_to_all(share, "blk", 0, 0, tiled=True)
    (gap,) = call(functools.partial(gap_kernel, samples, peers), [(1, 1)], [V, V])(share, norm)
    return dual.reshape(rows), margins.reshape(rows), gap.reshape(1)


def solution(mesh):
    placed = (P("blk", None), P("blk"), P("blk", None), P("grp"))
    return jax.shard_map(
        shards,
        mesh=mesh,
        in_specs=placed,
        out_specs=(P(("grp", "blk")), P(("grp", "blk")), P("grp")),
        check_vma=False,
    )
```

```python
import functools
import math

import jax
import jax.numpy as jnp
from jax import lax
from jax.experimental import pallas as pl
from jax.experimental.pallas import tpu as pltpu
from jax.sharding import PartitionSpec as P

ROUNDS = 2
HALF = 8
LOADS = 8
VMEM_LIMIT = 12 * 1024 * 1024

F32 = jnp.float32
BF16 = jnp.bfloat16
NT = (((1,), (1,)), ((), ()))
NN = (((1,), (0,)), ((), ()))


def regularization(reg_ref, samples):
    index = jnp.full((1, 1), reg_ref[0], jnp.int32).astype(F32)
    lam = 0.04 * jnp.exp(0.5 * math.log(2.0) * index)
    return lam, lam * samples


def ascend(gram, order_ref, signs, dual, score, reg_total, sigma, features):
    rows = gram.shape[0]
    blocks = order_ref.shape[1]
    eye = lax.broadcasted_iota(jnp.int32, (rows, rows), 0) == lax.broadcasted_iota(
        jnp.int32, (rows, rows), 1
    )
    block_of = lax.broadcasted_iota(jnp.int32, (1, rows), 1) // (rows // blocks)
    squared = jnp.sum(jnp.where(eye, gram, 0.0), axis=0, keepdims=True) / features + 1e-06
    rate = reg_total / (sigma * squared)
    couple = gram * (sigma / features / reg_total)
    change = jnp.zeros_like(dual)
    for position in range(blocks):
        current = dual + change
        updated = jnp.clip(current + rate * (1.0 - signs * score), 0.0, 1.0)
        step = jnp.where(block_of == order_ref[0, position], updated - current, 0.0)
        change = change + step
        if position < blocks - 1:
            coefficient = (signs * step).astype(BF16).astype(F32)
            column = jnp.sum(jnp.where(eye, coefficient, 0.0), axis=1, keepdims=True)
            score = score + jnp.sum(couple * column, axis=0, keepdims=True)
    return change


def weight_change(full, x_ref, keep_ref, send_ref, core, scale):
    rows, features = x_ref.shape
    segments = 2 * HALF
    length = features // segments
    depth = segments * rows
    spread = (
        lax.broadcasted_iota(jnp.int32, (rows, depth), 1) % rows
        == lax.broadcasted_iota(jnp.int32, (rows, depth), 0)
    )
    left = jnp.broadcast_to(full, (segments, rows)).astype(BF16)
    wide = lax.dot_general(
        left, jnp.where(spread, 1.0, 0.0).astype(BF16), NN, preferred_element_type=F32
    )
    segment_of = lax.broadcasted_iota(jnp.int32, (segments, depth), 1) // rows
    wanted = (lax.broadcasted_iota(jnp.int32, (segments, depth), 0) + core * HALF) % segments
    wide = jnp.where(segment_of == wanted, wide, 0.0).astype(BF16)
    width = min(length, 512)
    for begin in range(0, length, width):
        stacked = jnp.concatenate(
            [x_ref[:, g * length + begin : g * length + begin + width] for g in range(segments)],
            axis=0,
        )
        part = scale * lax.dot_general(wide, stacked, NN, preferred_element_type=F32)
        keep_ref[:, begin : begin + width] = part[:HALF]
        send_ref[:, begin : begin + width] = part[HALF:]


def scores(x_ref, low, high):
    rows, features = x_ref.shape
    segments = 2 * HALF
    length = features // segments
    total = jnp.zeros((HALF, rows), F32)
    row = lax.broadcasted_iota(jnp.int32, (HALF, rows), 0)
    for g in range(segments):
        half = low if g < HALF else high
        part = lax.dot_general(
            half, x_ref[:, g * length : (g + 1) * length], NT, preferred_element_type=F32
        )
        total = total + jnp.where(row == g % HALF, part, 0.0)
    return jnp.sum(total, axis=0, keepdims=True)


def first_kernel(samples, sigma, order_ref, reg_ref, core_ref, label_ref, data_ref,
                 keep_ref, send_ref, gram_ref, dual_ref, x_ref, arrived):
    rows, features = x_ref.shape
    width = features // LOADS
    copies = [
        pltpu.make_async_copy(
            data_ref.at[:, pl.ds(k * width, width)],
            x_ref.at[:, pl.ds(k * width, width)],
            arrived.at[k],
        )
        for k in range(LOADS)
    ]
    for copy in copies:
        copy.start()
    gram = jnp.zeros((rows, rows), F32)
    for k in range(LOADS):
        copies[k].wait()
        piece = x_ref[:, k * width : (k + 1) * width]
        gram = gram + lax.dot_general(piece, piece, NT, preferred_element_type=F32)
    gram_ref[...] = gram
    signs = label_ref[...].astype(F32)
    _, reg_total = regularization(reg_ref, samples)
    none = jnp.zeros((1, rows), F32)
    change = ascend(gram, order_ref, signs, none, none, reg_total, sigma, features)
    dual_ref[...] = change
    scale = 1.0 / math.sqrt(features) / reg_total
    weight_change((signs * change).astype(BF16), x_ref, keep_ref, send_ref, core_ref[0], scale)


def halves(own, other, core):
    low = jnp.where(core == 0, own, other)
    high = jnp.where(core == 0, other, own)
    return low, high


def next_kernel(samples, sigma, order_ref, reg_ref, core_ref, label_ref, own_ref, other_ref,
                gram_ref, old_dual_ref, x_ref, keep_ref, send_ref, dual_ref):
    rows, features = x_ref.shape
    signs = label_ref[...].astype(F32)
    _, reg_total = regularization(reg_ref, samples)
    low, high = halves(own_ref[...], other_ref[...], core_ref[0])
    score = 1.0 / math.sqrt(features) * scores(x_ref, low.astype(BF16), high.astype(BF16))
    dual = old_dual_ref[...]
    change = ascend(
        gram_ref[...], order_ref, signs, dual, score, reg_total, sigma, features
    )
    dual_ref[...] = dual + change
    scale = 1.0 / math.sqrt(features) / reg_total
    weight_change((signs * change).astype(BF16), x_ref, keep_ref, send_ref, core_ref[0], scale)


def last_kernel(samples, reg_ref, core_ref, label_ref, own_ref, other_ref, dual_ref, x_ref,
                margin_ref, share_ref, norm_ref):
    rows, features = x_ref.shape
    signs = label_ref[...].astype(F32)
    lam, _ = regularization(reg_ref, samples)
    low, high = halves(own_ref[...], other_ref[...], core_ref[0])
    margins = 1.0 / math.sqrt(features) * scores(x_ref, low.astype(BF16), high.astype(BF16))
    margin_ref[...] = margins
    hinge = jnp.maximum(0.0, 1.0 - signs * margins)
    share = jnp.sum(hinge - dual_ref[...], axis=1, keepdims=True)
    share_ref[...] = jnp.broadcast_to(share, share_ref.shape)
    norm = jnp.sum(low * low + high * high, axis=0, keepdims=True)
    norm_ref[...] = lam * jnp.sum(norm, axis=1, keepdims=True)


def gap_kernel(samples, peers, share_ref, norm_ref, gap_ref):
    total = share_ref[0:1, 0:1]
    step = share_ref.shape[0] // peers
    for k in range(1, peers):
        total = total + share_ref[k * step : k * step + 1, 0:1]
    gap_ref[...] = norm_ref[...] + total / samples


def swap(value, peers, partner):
    return lax.ppermute(value, "blk", [(i, partner(i)) for i in range(peers)])


def all_reduce(keep, send, peers):
    chips = peers // 2
    own = keep + swap(send, peers, lambda i: i ^ 1)
    mask = 1
    while mask < chips:
        own = own + swap(own, peers, lambda i: i ^ (2 * mask))
        mask = 2 * mask + 1
    return own, swap(own, peers, lambda i: i ^ 1)


def call(body, outs, spaces, scratch=()):
    return pl.pallas_call(
        body,
        out_shape=[jax.ShapeDtypeStruct(shape, dtype) for shape, dtype in outs],
        in_specs=[pl.BlockSpec(memory_space=space) for space in spaces],
        out_specs=[pl.BlockSpec(memory_space=pltpu.VMEM) for _ in outs],
        scratch_shapes=list(scratch),
        compiler_params=pltpu.CompilerParams(vmem_limit_bytes=VMEM_LIMIT),
    )


def shards(data, labels, order, reg_index):
    peers = lax.axis_size("blk")
    rows, features = data.shape
    samples = rows * peers
    sigma = float(peers)
    half = ((HALF, features // 2 // HALF), F32)
    core = (lax.axis_index("blk") % 2).astype(jnp.int32).reshape(1)
    label_row = labels.reshape(1, rows)
    S, V = pltpu.SMEM, pltpu.VMEM
    keep, send, gram, dual, near = call(
        functools.partial(first_kernel, samples, sigma),
        [half, half, ((rows, rows), F32), ((1, rows), F32), ((rows, features), BF16)],
        [S, S, S, V, pltpu.HBM],
        [pltpu.SemaphoreType.DMA((LOADS,))],
    )(order, reg_index, core, label_row, pltpu.with_memory_space_constraint(data, pltpu.HBM))
    own, other = all_reduce(keep, send, peers)
    for _ in range(ROUNDS - 1):
        keep, send, dual = call(
            functools.partial(next_kernel, samples, sigma),
            [half, half, ((1, rows), F32)],
            [S, S, S, V, V, V, V, V, V],
        )(order, reg_index, core, label_row, own, other, gram, dual, near)
        more, rest = all_reduce(keep, send, peers)
        own, other = own + more, other + rest
    margins, share, norm = call(
        functools.partial(last_kernel, samples),
        [((1, rows), F32), ((8 * peers, 128), F32), ((1, 1), F32)],
        [S, S, V, V, V, V, V],
    )(reg_index, core, label_row, own, other, dual, near)
    share = lax.all_to_all(share, "blk", 0, 0, tiled=True)
    (gap,) = call(functools.partial(gap_kernel, samples, peers), [((1, 1), F32)], [V, V])(share, norm)
    return dual.reshape(rows), margins.reshape(rows), gap.reshape(1)


def solution(mesh):
    placed = (P("blk", None), P("blk"), P("blk", None), P("grp"))
    return jax.shard_map(
        shards,
        mesh=mesh,
        in_specs=placed,
        out_specs=(P(("grp", "blk")), P(("grp", "blk")), P("grp")),
        check_vma=False,
    )
```

```python
import functools
import math

import jax
import jax.numpy as jnp
from jax import lax
from jax.experimental import pallas as pl
from jax.experimental.pallas import tpu as pltpu
from jax.sharding import PartitionSpec as P

ROUNDS = 2
SEGMENTS = 8
LOADS = 8
LANES = 128
VMEM_LIMIT = 12 * 1024 * 1024

F32 = jnp.float32
BF16 = jnp.bfloat16
NT = (((1,), (1,)), ((), ()))
NN = (((1,), (0,)), ((), ()))

SIGNS, VISIT, RATE, DUAL, FULL, TOTAL, STRENGTH = range(7)


def row_of(state_ref, row, count):
    return state_ref[row : row + 1, 0:count]


def ascend(couple, visit, blocks, signs, dual, rate, score):
    rows = couple.shape[0]
    eye = lax.broadcasted_iota(jnp.int32, (rows, rows), 0) == lax.broadcasted_iota(
        jnp.int32, (rows, rows), 1
    )
    change = jnp.zeros_like(dual)
    for position in range(blocks):
        current = dual + change
        updated = jnp.clip(current + rate * (1.0 - signs * score), 0.0, 1.0)
        step = jnp.where(visit == float(position), updated - current, 0.0)
        change = change + step
        if position < blocks - 1:
            coefficient = (signs * step).astype(BF16).astype(F32)
            column = jnp.sum(jnp.where(eye, coefficient, 0.0), axis=1, keepdims=True)
            score = score + jnp.sum(couple * column, axis=0, keepdims=True)
    return change


def weight_change(full, x_ref, out_ref, half, scale):
    rows, features = x_ref.shape
    length = features // 2 // SEGMENTS
    depth = SEGMENTS * rows
    spread = (
        lax.broadcasted_iota(jnp.int32, (rows, depth), 1) % rows
        == lax.broadcasted_iota(jnp.int32, (rows, depth), 0)
    )
    left = jnp.broadcast_to(full, (SEGMENTS, rows)).astype(BF16)
    wide = lax.dot_general(
        left, jnp.where(spread, 1.0, 0.0).astype(BF16), NN, preferred_element_type=F32
    )
    segment_of = lax.broadcasted_iota(jnp.int32, (SEGMENTS, depth), 1) // rows
    wanted = lax.broadcasted_iota(jnp.int32, (SEGMENTS, depth), 0)
    wide = jnp.where(segment_of == wanted, wide, 0.0).astype(BF16)
    width = min(length, 512)
    base = half * (features // 2)
    for begin in range(0, length, width):
        stacked = jnp.concatenate(
            [
                x_ref[:, pl.ds(pl.multiple_of(base + g * length + begin, LANES), width)]
                for g in range(SEGMENTS)
            ],
            axis=0,
        )
        out_ref[:, begin : begin + width] = scale * lax.dot_general(
            wide, stacked, NN, preferred_element_type=F32
        )


def scores(x_ref, weights, half):
    rows, features = x_ref.shape
    length = features // 2 // SEGMENTS
    base = half * (features // 2)
    weights = weights.astype(BF16)
    total = jnp.zeros((SEGMENTS, rows), F32)
    row = lax.broadcasted_iota(jnp.int32, (SEGMENTS, rows), 0)
    for g in range(SEGMENTS):
        part = lax.dot_general(
            weights,
            x_ref[:, pl.ds(pl.multiple_of(base + g * length, LANES), length)],
            NT,
            preferred_element_type=F32,
        )
        total = total + jnp.where(row == g, part, 0.0)
    return jnp.sum(total, axis=0, keepdims=True)


def core_index():
    return lax.rem(lax.axis_index("blk"), 2)


def first_kernel(samples, sigma, reg_ref, order_hbm, label_hbm, data_hbm,
                 send_ref, couple_ref, state_ref, x_ref,
                 order_ref, label_ref, arrived, small):
    rows, features = x_ref.shape
    blocks = order_ref.shape[1]
    width = features // LOADS
    copies = [
        pltpu.make_async_copy(
            data_hbm.at[:, pl.ds(k * width, width)],
            x_ref.at[:, pl.ds(k * width, width)],
            arrived.at[k],
        )
        for k in range(LOADS)
    ]
    for copy in copies:
        copy.start()
    fetches = [
        pltpu.make_async_copy(order_hbm, order_ref, small.at[0]),
        pltpu.make_async_copy(label_hbm, label_ref, small.at[1]),
    ]
    for fetch in fetches:
        fetch.start()
    gram = jnp.zeros((rows, rows), F32)
    for k in range(LOADS):
        copies[k].wait()
        piece = x_ref[:, k * width : (k + 1) * width]
        gram = gram + lax.dot_general(piece, piece, NT, preferred_element_type=F32)
    for fetch in fetches:
        fetch.wait()
    signs = label_ref[...].astype(F32)
    index = jnp.full((1, rows), reg_ref[0], jnp.int32).astype(F32)
    strength = 0.04 * jnp.exp(0.5 * math.log(2.0) * index)
    total = strength * samples
    block_of = lax.broadcasted_iota(jnp.int32, (1, rows), 1) // (rows // blocks)
    visit = jnp.zeros((1, rows), F32)
    for position in range(1, blocks):
        visit = jnp.where(block_of == order_ref[0, position], float(position), visit)
    eye = lax.broadcasted_iota(jnp.int32, (rows, rows), 0) == lax.broadcasted_iota(
        jnp.int32, (rows, rows), 1
    )
    squared = jnp.sum(jnp.where(eye, gram, 0.0), axis=0, keepdims=True) / features + 1e-06
    rate = total / (sigma * squared)
    couple = gram * (sigma / features / total)
    none = jnp.zeros((1, rows), F32)
    change = ascend(couple, visit, blocks, signs, none, rate, none)
    full = (signs * change).astype(BF16).astype(F32)
    couple_ref[...] = couple
    state_ref[...] = jnp.zeros_like(state_ref)
    for row, value in (
        (SIGNS, signs), (VISIT, visit), (RATE, rate), (DUAL, change),
        (FULL, full), (TOTAL, total), (STRENGTH, strength),
    ):
        state_ref[row : row + 1, 0:rows] = value
    scale = 1.0 / math.sqrt(features) / total[:, 0:1]
    weight_change(full, x_ref, send_ref, 1 - core_index(), scale)


def change_kernel(state_ref, x_ref, keep_ref):
    rows, features = x_ref.shape
    scale = 1.0 / math.sqrt(features) / row_of(state_ref, TOTAL, 1)
    weight_change(row_of(state_ref, FULL, rows), x_ref, keep_ref, core_index(), scale)


def score_kernel(own_ref, x_ref, part_ref):
    part_ref[...] = scores(x_ref, own_ref[...], core_index())


def next_kernel(blocks, part_ref, other_ref, couple_ref, state_ref, x_ref, send_ref, new_ref):
    rows, features = x_ref.shape
    signs = row_of(state_ref, SIGNS, rows)
    dual = row_of(state_ref, DUAL, rows)
    score = part_ref[...] + scores(x_ref, other_ref[...], 1 - core_index())
    score = 1.0 / math.sqrt(features) * score
    change = ascend(
        couple_ref[...], row_of(state_ref, VISIT, rows), blocks, signs, dual,
        row_of(state_ref, RATE, rows), score,
    )
    full = (signs * change).astype(BF16).astype(F32)
    new_ref[...] = state_ref[...]
    new_ref[DUAL : DUAL + 1, 0:rows] = dual + change
    new_ref[FULL : FULL + 1, 0:rows] = full
    scale = 1.0 / math.sqrt(features) / row_of(state_ref, TOTAL, 1)
    weight_change(full, x_ref, send_ref, 1 - core_index(), scale)


def last_kernel(part_ref, own_ref, other_ref, state_ref, x_ref, dual_ref, margin_ref, share_ref, norm_ref):
    rows, features = x_ref.shape
    signs = row_of(state_ref, SIGNS, rows)
    dual = row_of(state_ref, DUAL, rows)
    margins = part_ref[...] + scores(x_ref, other_ref[...], 1 - core_index())
    margins = 1.0 / math.sqrt(features) * margins
    hinge = jnp.maximum(0.0, 1.0 - signs * margins)
    share = jnp.sum(hinge - dual, axis=1, keepdims=True)
    share_ref[...] = jnp.broadcast_to(share, share_ref.shape)
    own, other = own_ref[...], other_ref[...]
    low = jnp.sum(jnp.sum(own * own, axis=0, keepdims=True), axis=1, keepdims=True)
    high = jnp.sum(jnp.sum(other * other, axis=0, keepdims=True), axis=1, keepdims=True)
    norm = row_of(state_ref, STRENGTH, 1) * (low + high)
    norm_ref[...] = jnp.broadcast_to(norm, norm_ref.shape)
    dual_ref[...] = dual
    margin_ref[...] = margins


def swap(value, peers, mask):
    return lax.ppermute(value, "blk", [(i, i ^ mask) for i in range(peers)])


def reduce_half(keep, arrived, peers):
    own = keep + arrived
    mask = 1
    while mask < peers // 2:
        own = own + swap(own, peers, 2 * mask)
        mask = 2 * mask + 1
    return own


def call(body, outs, spaces, scratch=(), work=0):
    return pl.pallas_call(
        body,
        out_shape=[jax.ShapeDtypeStruct(shape, dtype) for shape, dtype in outs],
        in_specs=[pl.BlockSpec(memory_space=space) for space in spaces],
        out_specs=[pl.BlockSpec(memory_space=pltpu.VMEM) for _ in outs],
        scratch_shapes=list(scratch),
        compiler_params=pltpu.CompilerParams(vmem_limit_bytes=VMEM_LIMIT),
        cost_estimate=pl.CostEstimate(flops=work, bytes_accessed=work // 64, transcendentals=0),
    )


def shards(data, labels, order, reg_index):
    peers = lax.axis_size("blk")
    rows, features = data.shape
    blocks = order.shape[1]
    samples = rows * peers
    work = 32 * rows * features
    half = ((SEGMENTS, features // 2 // SEGMENTS), F32)
    line = ((1, rows), F32)
    state_shape = ((8, LANES), F32)
    V, H = pltpu.VMEM, pltpu.HBM
    pinned = [
        pltpu.with_memory_space_constraint(a, H)
        for a in (order, labels.reshape(1, rows), data)
    ]
    send, couple, state, x = call(
        functools.partial(first_kernel, samples, float(peers)),
        [half, ((rows, rows), F32), state_shape, ((rows, features), BF16)],
        [pltpu.SMEM, H, H, H],
        [
            pltpu.SMEM(order.shape, jnp.int32),
            pltpu.VMEM((1, rows), jnp.int32),
            pltpu.SemaphoreType.DMA((LOADS,)),
            pltpu.SemaphoreType.DMA((2,)),
        ],
        work,
    )(reg_index, *pinned)
    own = None
    for index in range(ROUNDS):
        arrived = swap(send, peers, 1)
        (keep,) = call(change_kernel, [half], [V, V], work=work)(state, x)
        more = reduce_half(keep, arrived, peers)
        own = more if own is None else own + more
        other = swap(own, peers, 1)
        (part,) = call(score_kernel, [line], [V, V], work=work)(own, x)
        if index < ROUNDS - 1:
            send, state = call(
                functools.partial(next_kernel, blocks), [half, state_shape], [V] * 5, work=work
            )(part, other, couple, state, x)
    dual, margins, share, norm = call(
        last_kernel,
        [line, line, ((1, LANES), F32), ((1, LANES), F32)],
        [V] * 5,
        work=work,
    )(part, own, other, state, x)
    mask = 1
    while mask < peers:
        share = share + swap(share, peers, mask)
        mask *= 2
    gap = norm[0:1, 0:1] + share[0:1, 0:1] / samples
    return dual.reshape(rows), margins.reshape(rows), gap.reshape(1)


def solution(mesh):
    placed = (P("blk", None), P("blk"), P("blk", None), P("grp"))
    return jax.shard_map(
        shards,
        mesh=mesh,
        in_specs=placed,
        out_specs=(P(("grp", "blk")), P(("grp", "blk")), P("grp")),
        check_vma=False,
    )
```

```python
import functools
import math

import jax
import jax.numpy as jnp
from jax import lax
from jax.experimental import pallas as pl
from jax.experimental.pallas import tpu as pltpu
from jax.sharding import PartitionSpec as P

ROUNDS = 2
BLOCKS = 4
SEGMENTS = 8
LANES = 128
WIDTH = 1024
VMEM_LIMIT = 12 * 1024 * 1024

F32 = jnp.float32
BF16 = jnp.bfloat16
NT = (((1,), (1,)), ((), ()))
NN = (((1,), (0,)), ((), ()))

STRENGTH, TOTAL, SIGNS = 0, 1, 2
SQUARED, DUAL = SIGNS + BLOCKS, SIGNS + 2 * BLOCKS
PLACES = SIGNS + 3 * BLOCKS

def lane_iota(rows):
    return lax.broadcasted_iota(jnp.int32, (rows, LANES), 1)


def row_iota(rows):
    return lax.broadcasted_iota(jnp.int32, (rows, LANES), 0)


def stacked_block(x_ref, block, begin, width):
    size = LANES // (2 * SEGMENTS)
    length = x_ref.shape[1] // (2 * SEGMENTS)
    rows = pl.ds(pl.multiple_of(block * size, size), size)
    return jnp.concatenate(
        [x_ref[rows, g * length + begin : g * length + begin + width] for g in range(2 * SEGMENTS)],
        axis=0,
    )


def block_left(coefficient):
    size = coefficient.shape[0]
    line = jnp.sum(
        jnp.where(lane_iota(size) % size == row_iota(size), coefficient, 0.0), axis=0, keepdims=True
    )
    height = 2 * SEGMENTS
    return jnp.where(lane_iota(height) // size == row_iota(height), line, 0.0).astype(BF16)


def block_scores(product, size):
    height = product.shape[0]
    line = jnp.sum(
        jnp.where(lane_iota(height) // size == row_iota(height), product, 0.0), axis=0, keepdims=True
    )
    return jnp.sum(
        jnp.where(lane_iota(size) % size == row_iota(size), line, 0.0), axis=1, keepdims=True
    )


def block_step(signs, dual, squared, score, total, sigma):
    updated = jnp.clip(dual + total * (1.0 - signs * score) / (sigma * squared), 0.0, 1.0)
    return updated - dual


def advance(x_ref, local_ref, sum_ref, block, following, coefficient, rate, fresh):
    left = block_left(coefficient)
    length = local_ref.shape[1]
    width = min(length, WIDTH)
    product = jnp.zeros((2 * SEGMENTS, LANES), F32)
    for begin in range(0, length, width):
        columns = slice(begin, begin + width)
        update = lax.dot_general(
            left, stacked_block(x_ref, block, begin, width), NN, preferred_element_type=F32
        )
        sum_ref[:, columns] = update if fresh else sum_ref[:, columns] + update
        if following is not None:
            local = rate * update if local_ref is None else local_ref[:, columns] + rate * update
            local_ref[:, columns] = local
            product = product + lax.dot_general(
                local.astype(BF16),
                stacked_block(x_ref, following, begin, width),
                NT,
                preferred_element_type=F32,
            )
    return product


def scores(x_ref, weights, half):
    rows, features = x_ref.shape
    length = features // 2 // SEGMENTS
    base = half * (features // 2)
    weights = weights.astype(BF16)
    total = jnp.zeros((SEGMENTS, rows), F32)
    row = lax.broadcasted_iota(jnp.int32, (SEGMENTS, rows), 0)
    for g in range(SEGMENTS):
        part = lax.dot_general(
            weights,
            x_ref[:, pl.ds(pl.multiple_of(base + g * length, LANES), length)],
            NT,
            preferred_element_type=F32,
        )
        total = total + jnp.where(row == g, part, 0.0)
    return jnp.sum(total, axis=0, keepdims=True)


def core_index():
    return lax.rem(lax.axis_index("blk"), 2)


def split_halves(sum_ref, keep_ref, send_ref, scale):
    low = scale * sum_ref[0:SEGMENTS]
    high = scale * sum_ref[SEGMENTS : 2 * SEGMENTS]
    first = core_index() == 0
    keep_ref[...] = jnp.where(first, low, high)
    send_ref[...] = jnp.where(first, high, low)


def first_kernel(samples, sigma, reg_ref, order_hbm, label_hbm, data_hbm,
                 keep_ref, send_ref, state_ref, x_ref,
                 order_ref, label_ref, local_ref, sum_ref, arrived, small):
    rows, features = x_ref.shape
    blocks = order_ref.shape[1]
    size = rows // blocks
    fetch = pltpu.make_async_copy(order_hbm, order_ref, small.at[0])
    fetch.start()
    labels = pltpu.make_async_copy(label_hbm, label_ref, small.at[1])
    labels.start()
    fetch.wait()
    order = [order_ref[0, position] for position in range(blocks)]

    def load(position):
        place = pl.ds(pl.multiple_of(order[position] * size, size), size)
        return pltpu.make_async_copy(data_hbm.at[place], x_ref.at[place], arrived.at[position])

    for position in range(blocks):
        load(position).start()
    index = jnp.full((size, LANES), reg_ref[0], jnp.int32).astype(F32)
    strength = 0.04 * jnp.exp(0.5 * math.log(2.0) * index)
    total = strength * samples
    scale = 1.0 / math.sqrt(features)
    state_ref[STRENGTH] = strength
    state_ref[TOTAL] = total
    labels.wait()
    label_row = label_ref[...].astype(F32)
    spot = lax.broadcasted_iota(jnp.int32, (size, rows), 0)
    lane = lax.broadcasted_iota(jnp.int32, (size, rows), 1)
    for block in range(blocks):
        column = jnp.sum(
            jnp.where(lane == spot + block * size, label_row, 0.0), axis=1, keepdims=True
        )
        state_ref[SIGNS + block] = jnp.broadcast_to(column, (size, LANES))
    local_ref[...] = jnp.zeros_like(local_ref)
    score = jnp.zeros((size, LANES), F32)
    product = None
    for position in range(blocks):
        block = order[position]
        if position == 0:
            load(0).wait()
        place = pl.ds(pl.multiple_of(block * size, size), size)
        square = jnp.zeros((size, LANES), F32)
        for begin in range(0, features, LANES * 8):
            values = x_ref[place, begin : begin + LANES * 8].astype(F32)
            values = values * values
            for k in range(8):
                square = square + values[:, k * LANES : (k + 1) * LANES]
        squared = jnp.sum(square, axis=1, keepdims=True) / features + 1e-06
        squared = jnp.broadcast_to(squared, (size, LANES))
        state_ref[SQUARED + block] = squared
        if position > 0:
            score = jnp.broadcast_to(scale * block_scores(product, size), (size, LANES))
        signs = state_ref[SIGNS + block]
        step = block_step(signs, jnp.zeros_like(signs), squared, score, total, sigma)
        state_ref[DUAL + block] = step
        if position < blocks - 1:
            load(position + 1).wait()
        following = order[position + 1] if position < blocks - 1 else None
        product = advance(
            x_ref, local_ref, sum_ref, block, following, signs * step,
            (sigma * scale / total)[0:1, 0:1], position == 0,
        )
    split_halves(sum_ref, keep_ref, send_ref, (scale / total)[0:1, 0:1])


def score_norm_kernel(own_ref, x_ref, part_ref, norm_ref):
    own = own_ref[...]
    part_ref[...] = scores(x_ref, own, core_index())
    norm = jnp.sum(jnp.sum(own * own, axis=0, keepdims=True), axis=1, keepdims=True)
    norm_ref[...] = jnp.broadcast_to(norm, norm_ref.shape)


def next_kernel(samples, sigma, order_ref, own_ref, other_ref, state_ref, x_ref,
                keep_ref, send_ref, new_ref, local_ref, sum_ref):
    rows, features = x_ref.shape
    blocks = order_ref.shape[1]
    size = rows // blocks
    scale = 1.0 / math.sqrt(features)
    order = [order_ref[0, position] for position in range(blocks)]
    total = state_ref[TOTAL]
    new_ref[...] = state_ref[...]
    first = core_index() == 0
    local_ref[0:SEGMENTS] = jnp.where(first, own_ref[...], other_ref[...])
    local_ref[SEGMENTS : 2 * SEGMENTS] = jnp.where(first, other_ref[...], own_ref[...])
    length = local_ref.shape[1]
    width = min(length, WIDTH)
    product = jnp.zeros((2 * SEGMENTS, LANES), F32)
    for begin in range(0, length, width):
        product = product + lax.dot_general(
            local_ref[:, begin : begin + width].astype(BF16),
            stacked_block(x_ref, order[0], begin, width),
            NT,
            preferred_element_type=F32,
        )
    for position in range(blocks):
        block = order[position]
        score = jnp.broadcast_to(scale * block_scores(product, size), (size, LANES))
        signs = state_ref[SIGNS + block]
        dual = state_ref[DUAL + block]
        step = block_step(signs, dual, state_ref[SQUARED + block], score, total, sigma)
        new_ref[DUAL + block] = dual + step
        following = order[position + 1] if position < blocks - 1 else None
        product = advance(
            x_ref, local_ref, sum_ref, block, following, signs * step,
            (sigma * scale / total)[0:1, 0:1], position == 0,
        )
    split_halves(sum_ref, keep_ref, send_ref, (scale / total)[0:1, 0:1])


def rows_of(state_ref, start, blocks, size):
    rows = blocks * size
    lane = lax.broadcasted_iota(jnp.int32, (size, rows), 1)
    spot = lax.broadcasted_iota(jnp.int32, (size, rows), 0)
    line = jnp.zeros((1, rows), F32)
    for block in range(blocks):
        line = line + jnp.sum(
            jnp.where(lane == spot + block * size, state_ref[start + block][:, 0:rows], 0.0),
            axis=0, keepdims=True,
        )
    return line


def last_kernel(samples, chips, blocks, part_ref, norm_ref, other_ref, state_ref, x_ref,
                dual_ref, margin_ref, share_ref):
    rows, features = x_ref.shape
    size = rows // blocks
    signs = rows_of(state_ref, SIGNS, blocks, size)
    dual = rows_of(state_ref, DUAL, blocks, size)
    margins = part_ref[...] + scores(x_ref, other_ref[...], 1 - core_index())
    margins = 1.0 / math.sqrt(features) * margins
    hinge = jnp.maximum(0.0, 1.0 - signs * margins)
    share = jnp.sum(hinge - dual, axis=1, keepdims=True) / samples
    norm = state_ref[STRENGTH][0:1, 0:1] * norm_ref[:, 0:1] / chips
    share_ref[...] = jnp.broadcast_to(norm + share, share_ref.shape)
    dual_ref[...] = dual
    margin_ref[...] = margins


def swap(value, peers, mask):
    return lax.ppermute(value, "blk", [(i, i ^ mask) for i in range(peers)])


def reduce_half(keep, arrived, peers):
    own = keep + arrived
    mask = 1
    while mask < peers // 2:
        own = own + swap(own, peers, 2 * mask)
        mask = 2 * mask + 1
    return own


def sum_over_chips(value, peers):
    terms = [value] + [swap(value, peers, 2 * mask) for mask in range(1, peers // 2)]
    while len(terms) > 1:
        terms = [terms[k] + terms[k + 1] for k in range(0, len(terms), 2)]
    return terms[0]


def call(body, outs, spaces, scratch=(), work=0):
    return pl.pallas_call(
        body,
        out_shape=[jax.ShapeDtypeStruct(shape, dtype) for shape, dtype in outs],
        in_specs=[pl.BlockSpec(memory_space=space) for space in spaces],
        out_specs=[pl.BlockSpec(memory_space=pltpu.VMEM) for _ in outs],
        scratch_shapes=list(scratch),
        compiler_params=pltpu.CompilerParams(vmem_limit_bytes=VMEM_LIMIT),
        cost_estimate=pl.CostEstimate(flops=work, bytes_accessed=work // 64, transcendentals=0),
    )


def shards(data, labels, order, reg_index):
    peers = lax.axis_size("blk")
    rows, features = data.shape
    blocks = order.shape[1]
    samples = rows * peers
    work = 32 * rows * features
    length = features // 2 // SEGMENTS
    half = ((SEGMENTS, length), F32)
    line = ((1, rows), F32)
    scalar = ((1, LANES), F32)
    state_shape = ((PLACES, rows // blocks, LANES), F32)
    whole = pltpu.VMEM((2 * SEGMENTS, length), F32)
    S, V, H = pltpu.SMEM, pltpu.VMEM, pltpu.HBM
    pinned = [
        pltpu.with_memory_space_constraint(a, H) for a in (order, labels.reshape(1, rows), data)
    ]
    keep, send, state, x = call(
        functools.partial(first_kernel, samples, float(peers)),
        [half, half, state_shape, ((rows, features), BF16)],
        [S, H, H, H],
        [
            pltpu.SMEM(order.shape, jnp.int32),
            pltpu.VMEM((1, rows), jnp.int32),
            whole,
            whole,
            pltpu.SemaphoreType.DMA((blocks,)),
            pltpu.SemaphoreType.DMA((2,)),
        ],
        work,
    )(reg_index, *pinned)
    own = None
    for index in range(ROUNDS):
        more = reduce_half(keep, swap(send, peers, 1), peers)
        own = more if own is None else own + more
        other = swap(own, peers, 1)
        if index < ROUNDS - 1:
            keep, send, state = call(
                functools.partial(next_kernel, samples, float(peers)),
                [half, half, state_shape],
                [S, V, V, V, V],
                [whole, whole],
                work,
            )(order, own, other, state, x)
    part, norm = call(score_norm_kernel, [line, scalar], [V, V], work=work)(own, x)
    dual, margins, share = call(
        functools.partial(last_kernel, samples, peers // 2, blocks), [line, line, scalar], [V] * 5, work=work
    )(part, norm, other, state, x)
    mask = 1
    while mask < peers:
        share = share + swap(share, peers, mask)
        mask *= 2
    gap = share[0:1, 0:1]
    return dual.reshape(rows), margins.reshape(rows), gap.reshape(1)


def solution(mesh):
    placed = (P("blk", None), P("blk"), P("blk", None), P("grp"))
    return jax.shard_map(
        shards,
        mesh=mesh,
        in_specs=placed,
        out_specs=(P(("grp", "blk")), P(("grp", "blk")), P("grp")),
        check_vma=False,
    )
```

```python
import functools
import math

import jax
import jax.numpy as jnp
from jax import lax
from jax.experimental import pallas as pl
from jax.experimental.pallas import tpu as pltpu
from jax.sharding import PartitionSpec as P

ROUNDS = 2
BLOCKS = 4
LANES = 128
GROUP = 32
VMEM_LIMIT = 12 * 1024 * 1024

F32 = jnp.float32
BF16 = jnp.bfloat16
NT = (((1,), (1,)), ((), ()))
NN = (((1,), (0,)), ((), ()))

STRENGTH, TOTAL, SIGNS = 0, 1, 2
SQUARED, DUAL = SIGNS + BLOCKS, SIGNS + 2 * BLOCKS
PLACE, PIECES = SIGNS + 3 * BLOCKS, SIGNS + 4 * BLOCKS


def iota(shape, axis):
    return lax.broadcasted_iota(jnp.int32, shape, axis)


def block_left(coefficient):
    size = coefficient.shape[0]
    line = jnp.sum(
        jnp.where(iota((size, LANES), 1) % size == iota((size, LANES), 0), coefficient, 0.0),
        axis=0, keepdims=True,
    )
    shape = (GROUP, GROUP * size)
    wide = jnp.concatenate([line] * (GROUP * size // LANES), axis=1)
    return jnp.where(iota(shape, 1) // size == iota(shape, 0), wide, 0.0).astype(BF16)


def products(x_ref, block, weights, first, size):
    groups = weights.shape[0] // GROUP
    left = jnp.concatenate(
        [weights[g * GROUP : (g + 1) * GROUP] for g in range(groups)], axis=1
    ).astype(BF16)
    begin = first * size
    right = jnp.concatenate(
        [
            x_ref[block, pl.ds(begin + g * GROUP * size, GROUP * size), :]
            for g in range(groups)
        ],
        axis=1,
    )
    return lax.dot_general(left, right, NT, preferred_element_type=F32)


def same_tile(product, size):
    shape = product.shape
    line = jnp.sum(
        jnp.where(iota(shape, 1) // size == iota(shape, 0), product, 0.0), axis=0, keepdims=True
    )
    total = line[:, 0:LANES]
    for begin in range(LANES, shape[1], LANES):
        total = total + line[:, begin : begin + LANES]
    return total


def per_sample(line, size):
    column = jnp.sum(
        jnp.where(iota((size, LANES), 1) % size == iota((size, LANES), 0), line, 0.0),
        axis=1, keepdims=True,
    )
    return jnp.broadcast_to(column, (size, LANES))


def block_step(signs, dual, squared, score, total, sigma):
    updated = jnp.clip(dual + total * (1.0 - signs * score) / (sigma * squared), 0.0, 1.0)
    return updated - dual


def add_products(totals, x_ref, position, weights, round_ref, begin):
    size = totals[0].shape[0]
    rows = slice(begin, begin + GROUP)
    round_ref[rows] = weights.astype(BF16).astype(F32)
    values = x_ref[position, begin * size : (begin + GROUP) * size, :].astype(F32)
    totals = list(totals)
    for tile in range(GROUP):
        term = values[tile * size : (tile + 1) * size] * round_ref[begin + tile : begin + tile + 1]
        totals[tile % len(totals)] = totals[tile % len(totals)] + term
    return totals


def total_score(totals, scale):
    while len(totals) > 1:
        totals = [totals[k] + totals[k + 1] for k in range(0, len(totals), 2)]
    return jnp.broadcast_to(scale * jnp.sum(totals[0], axis=1, keepdims=True), totals[0].shape)


def no_totals(size):
    return [jnp.zeros((size, LANES), F32) for _ in range(4)]


def advance(x_ref, local_ref, sum_ref, round_ref, position, coefficient, rate, fresh, empty, onward):
    size = coefficient.shape[0]
    left = block_left(coefficient)
    totals = no_totals(size)
    for begin in range(0, sum_ref.shape[0], GROUP):
        rows = slice(begin, begin + GROUP)
        update = lax.dot_general(
            left,
            x_ref[position, begin * size : (begin + GROUP) * size, :],
            NN,
            preferred_element_type=F32,
        )
        sum_ref[rows] = update if fresh else sum_ref[rows] + update
        if onward:
            local = rate * update if empty else local_ref[rows] + rate * update
            local_ref[rows] = local
            totals = add_products(totals, x_ref, position + 1, local, round_ref, begin)
    return totals


def core_index():
    return lax.rem(lax.axis_index("blk"), 2)


def split_halves(sum_ref, keep_ref, send_ref, scale):
    half = keep_ref.shape[0]
    low = scale * sum_ref[0:half]
    high = scale * sum_ref[half : 2 * half]
    first = core_index() == 0
    keep_ref[...] = jnp.where(first, low, high)
    send_ref[...] = jnp.where(first, high, low)


def first_kernel(samples, sigma, reg_ref, order_hbm, label_hbm, data_hbm,
                 keep_ref, send_ref, state_ref, x_ref,
                 order_ref, label_ref, local_ref, sum_ref, round_ref, arrived, small):
    blocks = order_ref.shape[1]
    size = x_ref.shape[1] // sum_ref.shape[0]
    rows, features = blocks * size, sum_ref.shape[0] * LANES
    fetch = pltpu.make_async_copy(order_hbm, order_ref, small.at[0])
    fetch.start()
    labels = pltpu.make_async_copy(label_hbm, label_ref, small.at[1])
    labels.start()
    fetch.wait()
    order = [order_ref[0, position] for position in range(blocks)]

    def load(position):
        block = order[position]
        return pltpu.make_async_copy(data_hbm.at[block], x_ref.at[position], arrived.at[position])

    for position in range(blocks):
        load(position).start()
    index = jnp.full((size, LANES), reg_ref[0], jnp.int32).astype(F32)
    strength = 0.04 * jnp.exp(0.5 * math.log(2.0) * index)
    total = strength * samples
    scale = 1.0 / math.sqrt(features)
    state_ref[STRENGTH] = strength
    state_ref[TOTAL] = total
    labels.wait()
    label_row = label_ref[...].astype(F32)
    spot = lax.broadcasted_iota(jnp.int32, (size, rows), 0)
    lane = lax.broadcasted_iota(jnp.int32, (size, rows), 1)
    for position in range(blocks):
        begin = order[position] * size
        column = jnp.sum(jnp.where(lane == spot + begin, label_row, 0.0), axis=1, keepdims=True)
        state_ref[SIGNS + position] = jnp.broadcast_to(column, (size, LANES))
        state_ref[PLACE + position] = jnp.full((size, LANES), begin, jnp.int32).astype(F32)
    score = jnp.zeros((size, LANES), F32)
    for position in range(blocks):
        if position == 0:
            load(0).wait()
        square = no_totals(size)
        for begin in range(0, size * sum_ref.shape[0], 16 * size):
            values = x_ref[position, begin : begin + 16 * size, :].astype(F32)
            values = values * values
            for k in range(16):
                square[k % 4] = square[k % 4] + values[k * size : (k + 1) * size]
        squared = total_score(square, 1.0) / features + 1e-06
        state_ref[SQUARED + position] = squared
        if position > 0:
            score = total_score(totals, scale)
        signs = state_ref[SIGNS + position]
        step = block_step(signs, jnp.zeros_like(signs), squared, score, total, sigma)
        state_ref[DUAL + position] = step
        if position < blocks - 1:
            load(position + 1).wait()
        totals = advance(
            x_ref, local_ref, sum_ref, round_ref, position, signs * step,
            (sigma * scale / total)[0:1, 0:1], position == 0, position == 0, position < blocks - 1,
        )
    split_halves(sum_ref, keep_ref, send_ref, (scale / total)[0:1, 0:1])


def half_lines(x_ref, weights, core):
    blocks = x_ref.shape[0]
    half = weights.shape[0]
    size = x_ref.shape[1] // (2 * half)
    return [
        same_tile(products(x_ref, block, weights, core * half, size), size) for block in range(blocks)
    ]


def score_norm_kernel(own_ref, x_ref, part_ref, norm_ref):
    own = own_ref[...]
    lines = half_lines(x_ref, own, core_index())
    for block in range(len(lines)):
        part_ref[block : block + 1] = lines[block]
    norm = jnp.sum(jnp.sum(own * own, axis=0, keepdims=True), axis=1, keepdims=True)
    norm_ref[...] = jnp.broadcast_to(norm, norm_ref.shape)


def next_kernel(sigma, own_ref, other_ref, state_ref, x_ref,
                keep_ref, send_ref, new_ref, local_ref, sum_ref, round_ref):
    blocks = x_ref.shape[0]
    size = x_ref.shape[1] // sum_ref.shape[0]
    half = own_ref.shape[0]
    scale = 1.0 / math.sqrt(sum_ref.shape[0] * LANES)
    total = state_ref[TOTAL]
    new_ref[...] = state_ref[...]
    first = core_index() == 0
    totals = no_totals(size)
    for begin in range(0, 2 * half, GROUP):
        rows = slice(begin % half, begin % half + GROUP)
        own, other = own_ref[rows], other_ref[rows]
        if begin < half:
            local = jnp.where(first, own, other)
        else:
            local = jnp.where(first, other, own)
        local_ref[begin : begin + GROUP] = local
        totals = add_products(totals, x_ref, 0, local, round_ref, begin)
    for position in range(blocks):
        score = total_score(totals, scale)
        signs = state_ref[SIGNS + position]
        dual = state_ref[DUAL + position]
        step = block_step(signs, dual, state_ref[SQUARED + position], score, total, sigma)
        new_ref[DUAL + position] = dual + step
        totals = advance(
            x_ref, local_ref, sum_ref, round_ref, position, signs * step,
            (sigma * scale / total)[0:1, 0:1], position == 0, False, position < blocks - 1,
        )
    split_halves(sum_ref, keep_ref, send_ref, (scale / total)[0:1, 0:1])


def in_line(pieces, places):
    size = pieces[0].shape[0]
    shape = (size, len(pieces) * size)
    target = iota(shape, 1).astype(F32)
    spot = iota(shape, 0).astype(F32)
    line = jnp.zeros((1, shape[1]), F32)
    for piece, place in zip(pieces, places):
        here = target == spot + place[:, 0 : shape[1]]
        line = line + jnp.sum(jnp.where(here, piece[:, 0 : shape[1]], 0.0), axis=0, keepdims=True)
    return line


def last_kernel(samples, chips, part_ref, norm_ref, other_ref, state_ref, x_ref,
                dual_ref, margin_ref, share_ref):
    blocks = x_ref.shape[0]
    half = other_ref.shape[0]
    size = x_ref.shape[1] // (2 * half)
    scale = 1.0 / math.sqrt(2 * half * LANES)
    lines = half_lines(x_ref, other_ref[...], 1 - core_index())
    margins, spread = [], jnp.zeros((size, LANES), F32)
    for block in range(blocks):
        margins.append(scale * per_sample(part_ref[block : block + 1] + lines[block], size))
        hinge = jnp.maximum(0.0, 1.0 - state_ref[SIGNS + block] * margins[block])
        spread = spread + (hinge - state_ref[DUAL + block])
    share = jnp.sum(spread, axis=0, keepdims=True) / samples
    norm = state_ref[STRENGTH][0:1] * norm_ref[...] / chips
    share_ref[...] = norm + share
    places = [state_ref[PLACE + block] for block in range(blocks)]
    dual_ref[...] = in_line([state_ref[DUAL + block] for block in range(blocks)], places)
    margin_ref[...] = in_line(margins, places)


def swap(value, peers, mask):
    return lax.ppermute(value, "blk", [(i, i ^ mask) for i in range(peers)])


def reduce_half(keep, arrived, peers):
    own = keep + arrived
    mask = 1
    while mask < peers // 2:
        own = own + swap(own, peers, 2 * mask)
        mask = 2 * mask + 1
    return own


def sum_over_chips(value, peers):
    terms = [value] + [swap(value, peers, 2 * mask) for mask in range(1, peers // 2)]
    while len(terms) > 1:
        terms = [terms[k] + terms[k + 1] for k in range(0, len(terms), 2)]
    return terms[0]


def call(body, outs, spaces, scratch=(), work=0):
    return pl.pallas_call(
        body,
        out_shape=[jax.ShapeDtypeStruct(shape, dtype) for shape, dtype in outs],
        in_specs=[pl.BlockSpec(memory_space=space) for space in spaces],
        out_specs=[pl.BlockSpec(memory_space=pltpu.VMEM) for _ in outs],
        scratch_shapes=list(scratch),
        compiler_params=pltpu.CompilerParams(vmem_limit_bytes=VMEM_LIMIT),
        cost_estimate=pl.CostEstimate(flops=work, bytes_accessed=work // 64, transcendentals=0),
    )


def shards(data, labels, order, reg_index):
    peers = lax.axis_size("blk")
    rows, features = data.shape
    blocks = order.shape[1]
    samples = rows * peers
    work = 32 * rows * features
    size = rows // blocks
    tiles = features // LANES
    half = ((tiles // 2, LANES), F32)
    tiled = data.reshape(blocks, size, tiles, LANES).transpose(0, 2, 1, 3)
    tiled = tiled.reshape(blocks, tiles * size, LANES)
    line = ((1, rows), F32)
    scalar = ((1, LANES), F32)
    state_shape = ((PIECES, size, LANES), F32)
    whole = pltpu.VMEM((tiles, LANES), F32)
    S, V, H = pltpu.SMEM, pltpu.VMEM, pltpu.HBM
    pinned = [
        pltpu.with_memory_space_constraint(a, H) for a in (order, labels.reshape(1, rows), tiled)
    ]
    keep, send, state, x = call(
        functools.partial(first_kernel, samples, float(peers)),
        [half, half, state_shape, (tiled.shape, BF16)],
        [S, H, H, H],
        [
            pltpu.SMEM(order.shape, jnp.int32),
            pltpu.VMEM((1, rows), jnp.int32),
            whole,
            whole,
            whole,
            pltpu.SemaphoreType.DMA((blocks,)),
            pltpu.SemaphoreType.DMA((2,)),
        ],
        work,
    )(reg_index, *pinned)
    own = None
    for index in range(ROUNDS):
        more = reduce_half(keep, swap(send, peers, 1), peers)
        own = more if own is None else own + more
        other = swap(own, peers, 1)
        if index < ROUNDS - 1:
            keep, send, state = call(
                functools.partial(next_kernel, float(peers)),
                [half, half, state_shape],
                [V] * 4,
                [whole] * 3,
                work,
            )(own, other, state, x)
    part, norm = call(score_norm_kernel, [((blocks, LANES), F32), scalar], [V, V], work=work)(own, x)
    dual, margins, share = call(
        functools.partial(last_kernel, samples, peers // 2), [line, line, scalar], [V] * 5, work=work
    )(part, norm, other, state, x)
    mask = 1
    while mask < peers:
        share = share + swap(share, peers, mask)
        mask *= 2
    gap = share[0:1, 0:1]
    return dual.reshape(rows), margins.reshape(rows), gap.reshape(1)


def solution(mesh):
    placed = (P("blk", None), P("blk"), P("blk", None), P("grp"))
    return jax.shard_map(
        shards,
        mesh=mesh,
        in_specs=placed,
        out_specs=(P(("grp", "blk")), P(("grp", "blk")), P("grp")),
        check_vma=False,
    )
```

```python
import functools
import math

import jax
import jax.numpy as jnp
from jax import lax
from jax.experimental import pallas as pl
from jax.experimental.pallas import tpu as pltpu
from jax.sharding import PartitionSpec as P

ROUNDS = 2
BLOCKS = 4
LANES = 128
GROUP = 32
VMEM_LIMIT = 12 * 1024 * 1024

F32 = jnp.float32
BF16 = jnp.bfloat16
NN = (((1,), (0,)), ((), ()))

STRENGTH, TOTAL, SIGNS = 0, 1, 2
SQUARED, DUAL = SIGNS + BLOCKS, SIGNS + 2 * BLOCKS
PLACE, PIECES = SIGNS + 3 * BLOCKS, SIGNS + 4 * BLOCKS


def iota(shape, axis):
    return lax.broadcasted_iota(jnp.int32, shape, axis)


def block_left(coefficient):
    size = coefficient.shape[0]
    line = jnp.sum(
        jnp.where(iota((size, LANES), 1) % size == iota((size, LANES), 0), coefficient, 0.0),
        axis=0, keepdims=True,
    )
    shape = (GROUP, GROUP * size)
    wide = jnp.concatenate([line] * (GROUP * size // LANES), axis=1)
    return jnp.where(iota(shape, 1) // size == iota(shape, 0), wide, 0.0).astype(BF16)


def block_step(signs, dual, squared, score, total, sigma):
    updated = jnp.clip(dual + total * (1.0 - signs * score) / (sigma * squared), 0.0, 1.0)
    return updated - dual


def add_products(totals, x_ref, position, weights, round_ref, begin):
    size = totals[0].shape[0]
    rows = slice(begin, begin + GROUP)
    round_ref[rows] = weights.astype(BF16).astype(F32)
    values = x_ref[position, begin * size : (begin + GROUP) * size, :].astype(F32)
    totals = list(totals)
    for tile in range(GROUP):
        term = values[tile * size : (tile + 1) * size] * round_ref[begin + tile : begin + tile + 1]
        totals[tile % len(totals)] = totals[tile % len(totals)] + term
    return totals


def total_score(totals, scale):
    while len(totals) > 1:
        totals = [totals[k] + totals[k + 1] for k in range(0, len(totals), 2)]
    return jnp.broadcast_to(scale * jnp.sum(totals[0], axis=1, keepdims=True), totals[0].shape)


def no_totals(size):
    return [jnp.zeros((size, LANES), F32) for _ in range(4)]


def advance(x_ref, local_ref, sum_ref, round_ref, position, coefficient, rate, fresh, empty, onward):
    size = coefficient.shape[0]
    left = block_left(coefficient)
    totals = no_totals(size)
    for begin in range(0, sum_ref.shape[0], GROUP):
        rows = slice(begin, begin + GROUP)
        update = lax.dot_general(
            left,
            x_ref[position, begin * size : (begin + GROUP) * size, :],
            NN,
            preferred_element_type=F32,
        )
        sum_ref[rows] = update if fresh else sum_ref[rows] + update
        if onward:
            local = rate * update if empty else local_ref[rows] + rate * update
            local_ref[rows] = local
            totals = add_products(totals, x_ref, position + 1, local, round_ref, begin)
    return totals


def core_index():
    return lax.rem(lax.axis_index("blk"), 2)


def split_halves(sum_ref, keep_ref, send_ref, scale):
    half = keep_ref.shape[0]
    low = scale * sum_ref[0:half]
    high = scale * sum_ref[half : 2 * half]
    first = core_index() == 0
    keep_ref[...] = jnp.where(first, low, high)
    send_ref[...] = jnp.where(first, high, low)


def first_kernel(samples, sigma, reg_ref, order_hbm, label_hbm, data_hbm,
                 keep_ref, send_ref, state_ref, x_ref,
                 order_ref, label_ref, local_ref, sum_ref, round_ref, arrived, small):
    blocks = order_ref.shape[1]
    size = x_ref.shape[1] // sum_ref.shape[0]
    rows, features = blocks * size, sum_ref.shape[0] * LANES
    fetch = pltpu.make_async_copy(order_hbm, order_ref, small.at[0])
    fetch.start()
    labels = pltpu.make_async_copy(label_hbm, label_ref, small.at[1])
    labels.start()
    fetch.wait()
    order = [order_ref[0, position] for position in range(blocks)]

    def load(position):
        block = order[position]
        return pltpu.make_async_copy(data_hbm.at[block], x_ref.at[position], arrived.at[position])

    for position in range(blocks):
        load(position).start()
    index = jnp.full((size, LANES), reg_ref[0], jnp.int32).astype(F32)
    strength = 0.04 * jnp.exp(0.5 * math.log(2.0) * index)
    total = strength * samples
    scale = 1.0 / math.sqrt(features)
    state_ref[STRENGTH] = strength
    state_ref[TOTAL] = total
    labels.wait()
    label_row = label_ref[...].astype(F32)
    spot = lax.broadcasted_iota(jnp.int32, (size, rows), 0)
    lane = lax.broadcasted_iota(jnp.int32, (size, rows), 1)
    for position in range(blocks):
        begin = order[position] * size
        column = jnp.sum(jnp.where(lane == spot + begin, label_row, 0.0), axis=1, keepdims=True)
        state_ref[SIGNS + position] = jnp.broadcast_to(column, (size, LANES))
        state_ref[PLACE + position] = jnp.full((size, LANES), begin, jnp.int32).astype(F32)
    score = jnp.zeros((size, LANES), F32)
    for position in range(blocks):
        if position == 0:
            load(0).wait()
        square = no_totals(size)
        for begin in range(0, size * sum_ref.shape[0], 16 * size):
            values = x_ref[position, begin : begin + 16 * size, :].astype(F32)
            values = values * values
            for k in range(16):
                square[k % 4] = square[k % 4] + values[k * size : (k + 1) * size]
        squared = total_score(square, 1.0) / features + 1e-06
        state_ref[SQUARED + position] = squared
        if position > 0:
            score = total_score(totals, scale)
        signs = state_ref[SIGNS + position]
        step = block_step(signs, jnp.zeros_like(signs), squared, score, total, sigma)
        state_ref[DUAL + position] = step
        if position < blocks - 1:
            load(position + 1).wait()
        totals = advance(
            x_ref, local_ref, sum_ref, round_ref, position, signs * step,
            (sigma * scale / total)[0:1, 0:1], position == 0, position == 0, position < blocks - 1,
        )
    split_halves(sum_ref, keep_ref, send_ref, (scale / total)[0:1, 0:1])


def half_products(x_ref, weights_ref, round_ref, core):
    blocks = x_ref.shape[0]
    half = weights_ref.shape[0]
    size = x_ref.shape[1] // (2 * half)
    totals = [no_totals(size)[:2] for _ in range(blocks)]
    round_ref[...] = weights_ref[...].astype(BF16).astype(F32)
    for begin in range(0, half, GROUP):
        rows = pl.ds(pl.multiple_of((core * half + begin) * size, GROUP * size), GROUP * size)
        for block in range(blocks):
            values = x_ref[block, rows, :].astype(F32)
            for tile in range(GROUP):
                term = values[tile * size : (tile + 1) * size] * round_ref[begin + tile : begin + tile + 1]
                totals[block][tile % 2] = totals[block][tile % 2] + term
    return [first + second for first, second in totals]


def score_norm_kernel(own_ref, x_ref, part_ref, norm_ref, round_ref):
    own = own_ref[...]
    parts = half_products(x_ref, own_ref, round_ref, core_index())
    for block, part in enumerate(parts):
        part_ref[block] = part
    norm = jnp.sum(jnp.sum(own * own, axis=0, keepdims=True), axis=1, keepdims=True)
    norm_ref[...] = jnp.broadcast_to(norm, norm_ref.shape)


def next_kernel(sigma, own_ref, other_ref, state_ref, x_ref,
                keep_ref, send_ref, new_ref, local_ref, sum_ref, round_ref):
    blocks = x_ref.shape[0]
    size = x_ref.shape[1] // sum_ref.shape[0]
    half = own_ref.shape[0]
    scale = 1.0 / math.sqrt(sum_ref.shape[0] * LANES)
    total = state_ref[TOTAL]
    new_ref[...] = state_ref[...]
    first = core_index() == 0
    totals = no_totals(size)
    for begin in range(0, 2 * half, GROUP):
        rows = slice(begin % half, begin % half + GROUP)
        own, other = own_ref[rows], other_ref[rows]
        if begin < half:
            local = jnp.where(first, own, other)
        else:
            local = jnp.where(first, other, own)
        local_ref[begin : begin + GROUP] = local
        totals = add_products(totals, x_ref, 0, local, round_ref, begin)
    for position in range(blocks):
        score = total_score(totals, scale)
        signs = state_ref[SIGNS + position]
        dual = state_ref[DUAL + position]
        step = block_step(signs, dual, state_ref[SQUARED + position], score, total, sigma)
        new_ref[DUAL + position] = dual + step
        totals = advance(
            x_ref, local_ref, sum_ref, round_ref, position, signs * step,
            (sigma * scale / total)[0:1, 0:1], position == 0, False, position < blocks - 1,
        )
    split_halves(sum_ref, keep_ref, send_ref, (scale / total)[0:1, 0:1])


def in_line(pieces, places):
    size = pieces[0].shape[0]
    shape = (size, len(pieces) * size)
    target = iota(shape, 1).astype(F32)
    spot = iota(shape, 0).astype(F32)
    line = jnp.zeros((1, shape[1]), F32)
    for piece, place in zip(pieces, places):
        here = target == spot + place[:, 0 : shape[1]]
        line = line + jnp.sum(jnp.where(here, piece[:, 0 : shape[1]], 0.0), axis=0, keepdims=True)
    return line


def last_kernel(samples, chips, part_ref, norm_ref, other_ref, state_ref, x_ref,
                share_ref, margin_ref, round_ref):
    blocks = x_ref.shape[0]
    half = other_ref.shape[0]
    size = x_ref.shape[1] // (2 * half)
    scale = 1.0 / math.sqrt(2 * half * LANES)
    parts = half_products(x_ref, other_ref, round_ref, 1 - core_index())
    spread = jnp.zeros((size, LANES), F32)
    for block in range(blocks):
        margins = total_score([part_ref[block] + parts[block]], scale)
        margin_ref[block] = margins
        hinge = jnp.maximum(0.0, 1.0 - state_ref[SIGNS + block] * margins)
        spread = spread + (hinge - state_ref[DUAL + block])
    share = jnp.sum(spread, axis=0, keepdims=True) / samples
    share_ref[...] = state_ref[STRENGTH][0:1] * norm_ref[...] / chips + share


def line_kernel(state_ref, margin_ref, dual_ref, out_ref):
    blocks = margin_ref.shape[0]
    places = [state_ref[PLACE + block] for block in range(blocks)]
    dual_ref[...] = in_line([state_ref[DUAL + block] for block in range(blocks)], places)
    out_ref[...] = in_line([margin_ref[block] for block in range(blocks)], places)


def swap(value, peers, mask):
    return lax.ppermute(value, "blk", [(i, i ^ mask) for i in range(peers)])


def reduce_half(keep, arrived, peers):
    own = keep + arrived
    mask = 1
    while mask < peers // 2:
        own = own + swap(own, peers, 2 * mask)
        mask = 2 * mask + 1
    return own


def sum_over_chips(value, peers):
    terms = [value] + [swap(value, peers, 2 * mask) for mask in range(1, peers // 2)]
    while len(terms) > 1:
        terms = [terms[k] + terms[k + 1] for k in range(0, len(terms), 2)]
    return terms[0]


def call(body, outs, spaces, scratch=(), work=0):
    return pl.pallas_call(
        body,
        out_shape=[jax.ShapeDtypeStruct(shape, dtype) for shape, dtype in outs],
        in_specs=[pl.BlockSpec(memory_space=space) for space in spaces],
        out_specs=[pl.BlockSpec(memory_space=pltpu.VMEM) for _ in outs],
        scratch_shapes=list(scratch),
        compiler_params=pltpu.CompilerParams(vmem_limit_bytes=VMEM_LIMIT),
        cost_estimate=pl.CostEstimate(flops=work, bytes_accessed=work // 64, transcendentals=0),
    )


def shards(data, labels, order, reg_index):
    peers = lax.axis_size("blk")
    rows, features = data.shape
    blocks = order.shape[1]
    samples = rows * peers
    work = 32 * rows * features
    size = rows // blocks
    tiles = features // LANES
    half = ((tiles // 2, LANES), F32)
    tiled = data.reshape(blocks, size, tiles, LANES).transpose(0, 2, 1, 3)
    tiled = tiled.reshape(blocks, tiles * size, LANES)
    line = ((1, rows), F32)
    scalar = ((1, LANES), F32)
    state_shape = ((PIECES, size, LANES), F32)
    whole = pltpu.VMEM((tiles, LANES), F32)
    S, V, H = pltpu.SMEM, pltpu.VMEM, pltpu.HBM
    pinned = [
        pltpu.with_memory_space_constraint(a, H) for a in (order, labels.reshape(1, rows), tiled)
    ]
    keep, send, state, x = call(
        functools.partial(first_kernel, samples, float(peers)),
        [half, half, state_shape, (tiled.shape, BF16)],
        [S, H, H, H],
        [
            pltpu.SMEM(order.shape, jnp.int32),
            pltpu.VMEM((1, rows), jnp.int32),
            whole,
            whole,
            whole,
            pltpu.SemaphoreType.DMA((blocks,)),
            pltpu.SemaphoreType.DMA((2,)),
        ],
        work,
    )(reg_index, *pinned)
    own = None
    for index in range(ROUNDS):
        more = reduce_half(keep, swap(send, peers, 1), peers)
        own = more if own is None else own + more
        other = swap(own, peers, 1)
        if index < ROUNDS - 1:
            keep, send, state = call(
                functools.partial(next_kernel, float(peers)),
                [half, half, state_shape],
                [V] * 4,
                [whole] * 3,
                work,
            )(own, other, state, x)
    pieces = ((blocks, size, LANES), F32)
    rounded = [pltpu.VMEM((tiles // 2, LANES), F32)]
    part, norm = call(score_norm_kernel, [pieces, scalar], [V, V], rounded, work)(own, x)
    share, spread = call(
        functools.partial(last_kernel, samples, peers // 2), [scalar, pieces], [V] * 5, rounded, work
    )(part, norm, other, state, x)
    dual, margins = call(line_kernel, [line, line], [V] * 2, work=work)(state, spread)
    mask = 1
    while mask < peers:
        share = share + swap(share, peers, mask)
        mask *= 2
    gap = share[0:1, 0:1]
    return dual.reshape(rows), margins.reshape(rows), gap.reshape(1)


def solution(mesh):
    placed = (P("blk", None), P("blk"), P("blk", None), P("grp"))
    return jax.shard_map(
        shards,
        mesh=mesh,
        in_specs=placed,
        out_specs=(P(("grp", "blk")), P(("grp", "blk")), P("grp")),
        check_vma=False,
    )
```

```python
import functools
import math

import jax
import jax.numpy as jnp
from jax import lax
from jax.experimental import pallas as pl
from jax.experimental.pallas import tpu as pltpu
from jax.sharding import PartitionSpec as P

ROUNDS = 2
BLOCKS = 4
LANES = 128
GROUP = 16
VMEM_LIMIT = 12 * 1024 * 1024

F32 = jnp.float32
BF16 = jnp.bfloat16
NN = (((1,), (0,)), ((), ()))

STRENGTH, TOTAL, SIGNS = 0, 1, 2
SQUARED, DUAL = SIGNS + BLOCKS, SIGNS + 2 * BLOCKS
PLACE, PIECES = SIGNS + 3 * BLOCKS, SIGNS + 4 * BLOCKS


def iota(shape, axis):
    return lax.broadcasted_iota(jnp.int32, shape, axis)


def block_left(coefficient):
    size = coefficient.shape[0]
    line = jnp.sum(
        jnp.where(iota((size, LANES), 1) % size == iota((size, LANES), 0), coefficient, 0.0),
        axis=0, keepdims=True,
    )
    shape = (GROUP, GROUP * size)
    wide = jnp.concatenate([line] * (GROUP * size // LANES), axis=1)
    return jnp.where(iota(shape, 1) // size == iota(shape, 0), wide, 0.0).astype(BF16)


def block_step(signs, dual, squared, score, total, sigma):
    updated = jnp.clip(dual + total * (1.0 - signs * score) / (sigma * squared), 0.0, 1.0)
    return updated - dual


def add_products(totals, x_ref, position, weights, round_ref, begin):
    size = totals[0].shape[0]
    rows = slice(begin, begin + GROUP)
    round_ref[rows] = weights.astype(BF16).astype(F32)
    values = x_ref[position, begin * size : (begin + GROUP) * size, :].astype(F32)
    totals = list(totals)
    for tile in range(GROUP):
        term = values[tile * size : (tile + 1) * size] * round_ref[begin + tile : begin + tile + 1]
        totals[tile % len(totals)] = totals[tile % len(totals)] + term
    return totals


def total_score(totals, scale):
    while len(totals) > 1:
        totals = [totals[k] + totals[k + 1] for k in range(0, len(totals), 2)]
    return jnp.broadcast_to(scale * jnp.sum(totals[0], axis=1, keepdims=True), totals[0].shape)


def no_totals(size):
    return [jnp.zeros((size, LANES), F32) for _ in range(4)]


def advance(x_ref, local_ref, sum_ref, round_ref, position, coefficient, rate, fresh, empty, onward):
    size = coefficient.shape[0]
    left = block_left(coefficient)
    totals = no_totals(size)
    for begin in range(0, sum_ref.shape[0], GROUP):
        rows = slice(begin, begin + GROUP)
        update = lax.dot_general(
            left,
            x_ref[position, begin * size : (begin + GROUP) * size, :],
            NN,
            preferred_element_type=F32,
        )
        sum_ref[rows] = update if fresh else sum_ref[rows] + update
        if onward:
            local = rate * update if empty else local_ref[rows] + rate * update
            local_ref[rows] = local
            totals = add_products(totals, x_ref, position + 1, local, round_ref, begin)
    return totals


def core_index():
    return lax.rem(lax.axis_index("blk"), 2)


def split_halves(sum_ref, keep_ref, send_ref, scale):
    half = keep_ref.shape[0]
    low = scale * sum_ref[0:half]
    high = scale * sum_ref[half : 2 * half]
    first = core_index() == 0
    keep_ref[...] = jnp.where(first, low, high)
    send_ref[...] = jnp.where(first, high, low)


def first_kernel(samples, sigma, reg_ref, order_hbm, label_hbm, data_hbm,
                 keep_ref, send_ref, state_ref, x_ref,
                 order_ref, label_ref, local_ref, sum_ref, round_ref, arrived, small):
    blocks = order_ref.shape[1]
    size = x_ref.shape[1] // sum_ref.shape[0]
    rows, features = blocks * size, sum_ref.shape[0] * LANES
    fetch = pltpu.make_async_copy(order_hbm, order_ref, small.at[0])
    fetch.start()
    labels = pltpu.make_async_copy(label_hbm, label_ref, small.at[1])
    labels.start()
    fetch.wait()
    order = [order_ref[0, position] for position in range(blocks)]

    def load(position):
        block = order[position]
        return pltpu.make_async_copy(data_hbm.at[block], x_ref.at[position], arrived.at[position])

    for position in range(blocks):
        load(position).start()
    index = jnp.full((size, LANES), reg_ref[0], jnp.int32).astype(F32)
    strength = 0.04 * jnp.exp(0.5 * math.log(2.0) * index)
    total = strength * samples
    scale = 1.0 / math.sqrt(features)
    state_ref[STRENGTH] = strength
    state_ref[TOTAL] = total
    labels.wait()
    label_row = label_ref[...].astype(F32)
    spot = lax.broadcasted_iota(jnp.int32, (size, rows), 0)
    lane = lax.broadcasted_iota(jnp.int32, (size, rows), 1)
    for position in range(blocks):
        begin = order[position] * size
        column = jnp.sum(jnp.where(lane == spot + begin, label_row, 0.0), axis=1, keepdims=True)
        state_ref[SIGNS + position] = jnp.broadcast_to(column, (size, LANES))
        state_ref[PLACE + position] = jnp.full((size, LANES), begin, jnp.int32).astype(F32)
    score = jnp.zeros((size, LANES), F32)
    for position in range(blocks):
        if position == 0:
            load(0).wait()
        square = no_totals(size)
        for begin in range(0, size * sum_ref.shape[0], 16 * size):
            values = x_ref[position, begin : begin + 16 * size, :].astype(F32)
            values = values * values
            for k in range(16):
                square[k % 4] = square[k % 4] + values[k * size : (k + 1) * size]
        squared = total_score(square, 1.0) / features + 1e-06
        state_ref[SQUARED + position] = squared
        if position > 0:
            score = total_score(totals, scale)
        signs = state_ref[SIGNS + position]
        step = block_step(signs, jnp.zeros_like(signs), squared, score, total, sigma)
        state_ref[DUAL + position] = step
        if position < blocks - 1:
            load(position + 1).wait()
        totals = advance(
            x_ref, local_ref, sum_ref, round_ref, position, signs * step,
            (sigma * scale / total)[0:1, 0:1], position == 0, position == 0, position < blocks - 1,
        )
    split_halves(sum_ref, keep_ref, send_ref, (scale / total)[0:1, 0:1])


def half_products(x_ref, weights_ref, round_ref, core):
    blocks = x_ref.shape[0]
    half = weights_ref.shape[0]
    size = x_ref.shape[1] // (2 * half)
    totals = [no_totals(size)[:2] for _ in range(blocks)]
    round_ref[...] = weights_ref[...].astype(BF16).astype(F32)
    for begin in range(0, half, GROUP):
        rows = pl.ds(pl.multiple_of((core * half + begin) * size, GROUP * size), GROUP * size)
        for block in range(blocks):
            values = x_ref[block, rows, :].astype(F32)
            for tile in range(GROUP):
                term = values[tile * size : (tile + 1) * size] * round_ref[begin + tile : begin + tile + 1]
                totals[block][tile % 2] = totals[block][tile % 2] + term
    return [first + second for first, second in totals]


def score_norm_kernel(own_ref, x_ref, part_ref, norm_ref, round_ref):
    own = own_ref[...]
    parts = half_products(x_ref, own_ref, round_ref, core_index())
    for block, part in enumerate(parts):
        part_ref[block] = part
    norm = jnp.sum(jnp.sum(own * own, axis=0, keepdims=True), axis=1, keepdims=True)
    norm_ref[...] = jnp.broadcast_to(norm, norm_ref.shape)


def next_kernel(sigma, own_ref, other_ref, state_ref, x_ref,
                keep_ref, send_ref, new_ref, local_ref, sum_ref, round_ref):
    blocks = x_ref.shape[0]
    size = x_ref.shape[1] // sum_ref.shape[0]
    half = own_ref.shape[0]
    scale = 1.0 / math.sqrt(sum_ref.shape[0] * LANES)
    total = state_ref[TOTAL]
    new_ref[...] = state_ref[...]
    first = core_index() == 0
    totals = no_totals(size)
    for begin in range(0, 2 * half, GROUP):
        rows = slice(begin % half, begin % half + GROUP)
        own, other = own_ref[rows], other_ref[rows]
        if begin < half:
            local = jnp.where(first, own, other)
        else:
            local = jnp.where(first, other, own)
        local_ref[begin : begin + GROUP] = local
        totals = add_products(totals, x_ref, 0, local, round_ref, begin)
    for position in range(blocks):
        score = total_score(totals, scale)
        signs = state_ref[SIGNS + position]
        dual = state_ref[DUAL + position]
        step = block_step(signs, dual, state_ref[SQUARED + position], score, total, sigma)
        new_ref[DUAL + position] = dual + step
        totals = advance(
            x_ref, local_ref, sum_ref, round_ref, position, signs * step,
            (sigma * scale / total)[0:1, 0:1], position == 0, False, position < blocks - 1,
        )
    split_halves(sum_ref, keep_ref, send_ref, (scale / total)[0:1, 0:1])


def in_line(pieces, places):
    size = pieces[0].shape[0]
    shape = (size, len(pieces) * size)
    target = iota(shape, 1).astype(F32)
    spot = iota(shape, 0).astype(F32)
    line = jnp.zeros((1, shape[1]), F32)
    for piece, place in zip(pieces, places):
        here = target == spot + place[:, 0 : shape[1]]
        line = line + jnp.sum(jnp.where(here, piece[:, 0 : shape[1]], 0.0), axis=0, keepdims=True)
    return line


def last_kernel(samples, chips, part_ref, norm_ref, other_ref, state_ref, x_ref,
                share_ref, margin_ref, round_ref):
    blocks = x_ref.shape[0]
    half = other_ref.shape[0]
    size = x_ref.shape[1] // (2 * half)
    scale = 1.0 / math.sqrt(2 * half * LANES)
    parts = half_products(x_ref, other_ref, round_ref, 1 - core_index())
    spread = jnp.zeros((size, LANES), F32)
    for block in range(blocks):
        margins = total_score([part_ref[block] + parts[block]], scale)
        margin_ref[block] = margins
        hinge = jnp.maximum(0.0, 1.0 - state_ref[SIGNS + block] * margins)
        spread = spread + (hinge - state_ref[DUAL + block])
    share = jnp.sum(spread, axis=0, keepdims=True) / samples
    share_ref[...] = state_ref[STRENGTH][0:1] * norm_ref[...] / chips + share


def line_kernel(state_ref, margin_ref, dual_ref, out_ref):
    blocks = margin_ref.shape[0]
    places = [state_ref[PLACE + block] for block in range(blocks)]
    dual_ref[...] = in_line([state_ref[DUAL + block] for block in range(blocks)], places)
    out_ref[...] = in_line([margin_ref[block] for block in range(blocks)], places)


def swap(value, peers, mask):
    return lax.ppermute(value, "blk", [(i, i ^ mask) for i in range(peers)])


def reduce_half(keep, arrived, peers):
    own = keep + arrived
    mask = 1
    while mask < peers // 2:
        own = own + swap(own, peers, 2 * mask)
        mask = 2 * mask + 1
    return own


def sum_over_chips(value, peers):
    terms = [value] + [swap(value, peers, 2 * mask) for mask in range(1, peers // 2)]
    while len(terms) > 1:
        terms = [terms[k] + terms[k + 1] for k in range(0, len(terms), 2)]
    return terms[0]


def call(body, outs, spaces, scratch=(), work=0):
    return pl.pallas_call(
        body,
        out_shape=[jax.ShapeDtypeStruct(shape, dtype) for shape, dtype in outs],
        in_specs=[pl.BlockSpec(memory_space=space) for space in spaces],
        out_specs=[pl.BlockSpec(memory_space=pltpu.VMEM) for _ in outs],
        scratch_shapes=list(scratch),
        compiler_params=pltpu.CompilerParams(vmem_limit_bytes=VMEM_LIMIT),
        cost_estimate=pl.CostEstimate(flops=work, bytes_accessed=work // 64, transcendentals=0),
    )


def shards(data, labels, order, reg_index):
    peers = lax.axis_size("blk")
    rows, features = data.shape
    blocks = order.shape[1]
    samples = rows * peers
    work = 32 * rows * features
    size = rows // blocks
    tiles = features // LANES
    half = ((tiles // 2, LANES), F32)
    tiled = data.reshape(blocks, size, tiles, LANES).transpose(0, 2, 1, 3)
    tiled = tiled.reshape(blocks, tiles * size, LANES)
    line = ((1, rows), F32)
    scalar = ((1, LANES), F32)
    state_shape = ((PIECES, size, LANES), F32)
    whole = pltpu.VMEM((tiles, LANES), F32)
    S, V, H = pltpu.SMEM, pltpu.VMEM, pltpu.HBM
    pinned = [
        pltpu.with_memory_space_constraint(a, H) for a in (order, labels.reshape(1, rows), tiled)
    ]
    keep, send, state, x = call(
        functools.partial(first_kernel, samples, float(peers)),
        [half, half, state_shape, (tiled.shape, BF16)],
        [S, H, H, H],
        [
            pltpu.SMEM(order.shape, jnp.int32),
            pltpu.VMEM((1, rows), jnp.int32),
            whole,
            whole,
            whole,
            pltpu.SemaphoreType.DMA((blocks,)),
            pltpu.SemaphoreType.DMA((2,)),
        ],
        work,
    )(reg_index, *pinned)
    own = None
    for index in range(ROUNDS):
        more = reduce_half(keep, swap(send, peers, 1), peers)
        own = more if own is None else own + more
        other = swap(own, peers, 1)
        if index < ROUNDS - 1:
            keep, send, state = call(
                functools.partial(next_kernel, float(peers)),
                [half, half, state_shape],
                [V] * 4,
                [whole] * 3,
                work,
            )(own, other, state, x)
    pieces = ((blocks, size, LANES), F32)
    rounded = [pltpu.VMEM((tiles // 2, LANES), F32)]
    part, norm = call(score_norm_kernel, [pieces, scalar], [V, V], rounded, work)(own, x)
    share, spread = call(
        functools.partial(last_kernel, samples, peers // 2), [scalar, pieces], [V] * 5, rounded, work
    )(part, norm, other, state, x)
    dual, margins = call(line_kernel, [line, line], [V] * 2, work=work)(state, spread)
    mask = 1
    while mask < peers:
        share = share + swap(share, peers, mask)
        mask *= 2
    gap = share[0:1, 0:1]
    return dual.reshape(rows), margins.reshape(rows), gap.reshape(1)


def solution(mesh):
    placed = (P("blk", None), P("blk"), P("blk", None), P("grp"))
    return jax.shard_map(
        shards,
        mesh=mesh,
        in_specs=placed,
        out_specs=(P(("grp", "blk")), P(("grp", "blk")), P("grp")),
        check_vma=False,
    )
```
